32 devices in a mesh: root: 4 (over z), virt: 4 (over y, x), occ: 2 (over core).
Axes of the slice: x: 2, y: 2, z: 4, core: 2. Of those that a mesh axis runs over, the one named last changes fastest.
Arguments:
- trial_singles: bfloat16 [8, 96], P('root'), may hold values from -6 to 6
- trial_doubles: bfloat16 [8, 480, 9216], P('root', 'virt', 'occ'), may hold values from -6 to 6
- occ_fock: bfloat16 [96, 96], replicated, may hold values from -0.625 to 0.625
- virt_fock: bfloat16 [480, 480], replicated, may hold values from -0.25 to 0.25
- w_ovoo: bfloat16 [96, 480, 9216], P('occ', 'virt', 'root'), may hold values from -0.625 to 0.625
- w_ooov: bfloat16 [96, 480, 9216], P('occ', 'virt', 'root'), may hold values from -0.0029296875 to 0.0029296875
- converged: int32 [8], replicated, may hold values from 0 to 1, as said below
Outputs:
- sigma_doubles: bfloat16 [8, 480, 9216], P('root', 'virt', 'occ')
- sigma_singles: float32 [8, 96], P('root')
- subspace: float32 [8, 8], P('root')
The draws below stay inside these ranges and needn't reach their ends.
Inputs may be any that keep to these rules, and one draw needn't show every extreme that they name: `converged`: exactly 4 roots are active (0). In every draw at least one aligned block of 2 roots has all its roots active; other blocks may have none.
All inputs are finite; a program needn't handle non-finite values.
Results may differ from the reference program's by a relative error of at most 0.0044.
Values may be sent and summed in bfloat16 or wider, within the bound.
A program may use at most 256 MiB of HBM per device.

```python
import math
import jax
import jax.numpy as jnp
from jax import lax

O = 96
V = 480
ROOTS_DEV = 2
ROOTS = 8


def draw_converged(key, part):
    groups = ROOTS // ROOTS_DEV
    level = jax.random.randint(jax.random.fold_in(key, 11), (groups,), 0, 4)
    chosen = jax.random.randint(jax.random.fold_in(key, 13), (), 0, groups)
    level = level.at[chosen].set(4)
    noise = jax.random.randint(jax.random.fold_in(key, 12), (ROOTS,), 0, ROOTS)
    positions = jnp.arange(ROOTS, dtype=jnp.int32)
    group_of = positions // ROOTS_DEV
    score = (level[group_of] * ROOTS + noise) * ROOTS + positions
    ranking = jnp.argsort(jnp.argsort(-score))
    return (ranking >= ROOTS // 2).astype(jnp.int32)


def levels(rng, dims, shards, low, high):
    def one(position, parts):
        draws = jax.random.uniform(jax.random.fold_in(jax.random.fold_in(rng, 6), position), (parts,), jnp.float32, low / len(shards), high / len(shards))
        return jnp.repeat(jnp.exp(draws), dims[position] // parts).reshape((-1,) + (1,) * (len(dims) - position - 1))

    gain = one(*shards[0])
    for cut in shards[1:]:
        gain = gain * one(*cut)
    return gain


def scatter_about(stream_key, extent, width, limit, cuts=(), kind=jnp.bfloat16):
    loudness = levels(stream_key, extent, cuts, -0.22, 0.18) if cuts else 1.0
    values = jax.random.normal(stream_key, extent, jnp.float32) * width * loudness
    return jnp.minimum(jnp.maximum(values, -limit), limit).astype(kind)


def setup_inputs(seed: int = 0) -> dict:
    streams_of = jax.random.split(jax.random.key(seed), 8)
    trial_singles = scatter_about(streams_of[0], (ROOTS, O), 1.0, 6.0, ((0, 4),))
    trial_doubles = scatter_about(streams_of[1], (ROOTS, V, O * O), 1.0, 6.0, ((0, 4), (1, 4), (2, 2)))
    occ_fock = scatter_about(streams_of[2], (O, O), O ** -0.5, 0.625)
    virt_fock = scatter_about(streams_of[3], (V, V), V ** -0.5, 0.25)
    w_ovoo = scatter_about(streams_of[4], (O, V, O * O), O ** -0.5, 0.625, ((0, 2), (1, 4), (2, 4)))
    w_ooov = scatter_about(streams_of[5], (O, V, O * O), (O * O * V) ** -0.5, 0.0029296875, ((0, 2), (1, 4), (2, 4)))
    converged = draw_converged(jax.random.fold_in(streams_of[7], 71), 0)
    return {"trial_singles": trial_singles, "trial_doubles": trial_doubles, "occ_fock": occ_fock, "virt_fock": virt_fock, "w_ovoo": w_ovoo, "w_ooov": w_ooov, "converged": converged}


def reference(trial_singles, trial_doubles, occ_fock, virt_fock, w_ovoo, w_ooov, converged):
    active = (1 - converged).astype(jnp.float32)
    outer_flat = w_ovoo.reshape(O, V * O * O)
    inner_flat = w_ooov.reshape(O, V * O * O)
    occ_wide = occ_fock.astype(jnp.float32)

    def per_root(bundle):
        single_row, double_block, weight_now = bundle
        outer_term = (-jnp.dot(single_row[None, :], outer_flat, preferred_element_type=jnp.float32)).reshape(V, O, O)
        vv_term = jnp.dot(virt_fock, double_block, preferred_element_type=jnp.float32).astype(jnp.bfloat16).reshape(V, O, O)
        block_wide = double_block.reshape(V, O, O).astype(jnp.float32)
        first_term = jnp.einsum('ki,akj->aij', occ_wide, block_wide)
        second_term = jnp.einsum('kj,aik->aij', occ_wide, block_wide)
        summed = weight_now * (vv_term.astype(jnp.float32) + outer_term - first_term - second_term)
        coupling = jnp.dot(inner_flat, double_block.reshape(V * O * O), preferred_element_type=jnp.float32)
        return (summed.reshape(V, O * O).astype(jnp.bfloat16), coupling)
    sigma_doubles, coupling = lax.map(per_root, (trial_singles, trial_doubles, active))
    singles_fock = jnp.dot(trial_singles, occ_fock, preferred_element_type=jnp.float32)
    sigma_singles = active[:, None] * (-singles_fock - 0.5 * coupling)
    doubles_part = jnp.dot(trial_doubles.reshape(ROOTS, V * O * O), sigma_doubles.reshape(ROOTS, V * O * O).T, preferred_element_type=jnp.float32)
    singles_part = jnp.dot(trial_singles.astype(jnp.float32), sigma_singles.T, precision=lax.Precision.HIGHEST)
    subspace = doubles_part / math.sqrt(O * O * V) + singles_part / math.sqrt(O)
    return (sigma_doubles, sigma_singles, subspace)
```

```python
import functools
import math

import jax
import jax.numpy as jnp
from jax import lax
from jax.experimental import pallas as pl
from jax.experimental.pallas import tpu as pltpu
from jax.sharding import PartitionSpec as P


def flat_pairs(left, right):
    return lax.dot_general(
        left.reshape(left.shape[0], -1),
        right.reshape(right.shape[0], -1),
        (((1,), (1,)), ((), ())),
        preferred_element_type=jnp.float32,
    )


def plain(trial_singles, trial_doubles, occ_fock, virt_fock, w_ovoo, w_ooov, converged):
    local_roots, virt_local, pair_local = trial_doubles.shape
    occ_count = occ_fock.shape[0]
    virt_count = virt_fock.shape[0]
    root_count = converged.shape[0]
    root_groups = lax.axis_size("root")
    occ_groups = lax.axis_size("occ")
    root_index = lax.axis_index("root")
    occ_index = lax.axis_index("occ")
    occ_half = occ_count // occ_groups
    block_pairs = occ_count * occ_count // root_groups
    own_start = occ_index * occ_half
    active = (1 - converged).astype(jnp.float32)
    own_active = lax.dynamic_slice_in_dim(active, root_index * local_roots, local_roots)
    singles_all = lax.all_gather(trial_singles, "root", axis=0, tiled=True)
    gathered = lax.all_gather(trial_doubles, "occ", axis=2, tiled=True)
    fock_cols = lax.dynamic_slice_in_dim(occ_fock, own_start, occ_half, 1)
    batch_rows = local_roots * virt_local
    stacked = gathered.reshape(batch_rows, occ_count, occ_count)
    first_term = jnp.einsum(
        "ki,bkj->bij", fock_cols, stacked, preferred_element_type=jnp.float32
    ).reshape(local_roots, virt_local, pair_local)
    own_rows = trial_doubles.reshape(batch_rows, occ_half, occ_count)
    second_term = jnp.einsum(
        "bik,kj->bij", own_rows, occ_fock, preferred_element_type=jnp.float32
    ).reshape(local_roots, virt_local, pair_local)
    doubles_block = lax.all_to_all(gathered, "root", split_axis=2, concat_axis=0, tiled=True)
    partial_coupling = flat_pairs(doubles_block, w_ooov)
    coupling_part = lax.dynamic_update_slice(
        jnp.zeros((root_count, occ_count), jnp.float32), partial_coupling, (jnp.int32(0), own_start)
    )
    coupling = lax.psum(coupling_part, ("root", "virt", "occ"))
    singles_fock = jnp.dot(singles_all, occ_fock, preferred_element_type=jnp.float32)
    singles_every = active[:, None] * (-singles_fock - 0.5 * coupling)
    sigma_singles = lax.dynamic_slice_in_dim(singles_every, root_index * local_roots, local_roots)
    singles_cols = lax.dynamic_slice_in_dim(singles_all, own_start, occ_half, 1)
    outer_part = (
        -jnp.dot(singles_cols, w_ovoo.reshape(occ_half, -1), preferred_element_type=jnp.float32)
    ).reshape(root_count, virt_local, block_pairs)
    product = jnp.einsum(
        "ac,ncp->nap",
        virt_fock,
        lax.all_to_all(trial_doubles, "virt", split_axis=2, concat_axis=1, tiled=True),
        preferred_element_type=jnp.float32,
    ).astype(jnp.bfloat16)
    vv_term = lax.all_to_all(product, "virt", split_axis=1, concat_axis=2, tiled=True)
    vv_value = vv_term.astype(jnp.float32)
    outer_own = lax.all_to_all(outer_part, "root", split_axis=0, concat_axis=2, tiled=True)
    outer_half = lax.psum_scatter(outer_own, "occ", scatter_dimension=2, tiled=True)
    summed = vv_value + outer_half - first_term - second_term
    sigma_doubles = (own_active[:, None, None] * summed).astype(jnp.bfloat16)
    trial_piece, sigma_piece = (
        lax.all_to_all(trial_doubles, "root", split_axis=2, concat_axis=0, tiled=True),
        lax.all_to_all(sigma_doubles, "root", split_axis=2, concat_axis=0, tiled=True),
    )
    doubles_part = lax.psum(flat_pairs(trial_piece, sigma_piece), ("root", "virt", "occ"))
    singles_part = jnp.dot(
        singles_all.astype(jnp.float32), singles_every.T, precision=lax.Precision.HIGHEST
    )
    whole_matrix = doubles_part / math.sqrt(
        occ_count * occ_count * virt_count
    ) + singles_part / math.sqrt(occ_count)
    subspace = lax.dynamic_slice_in_dim(whole_matrix, root_index * local_roots, local_roots, 0)
    return (sigma_doubles, sigma_singles, subspace)


ROWS = 8
MESH = pl.DeviceIdType.MESH
HIGH = lax.Precision.HIGHEST
CORES = 2


def flat(block):
    count, rows, width = block.shape
    return block.astype(jnp.float32).reshape(count * rows, width).astype(jnp.bfloat16)


def iota(shape, axis):
    return lax.broadcasted_iota(jnp.int32, shape, axis)


def one_hot(mask, dtype=jnp.float32):
    return jnp.where(mask, 1.0, 0.0).astype(dtype)


def dot(left, right, precision=None):
    return jnp.dot(left, right, preferred_element_type=jnp.float32, precision=precision)


def dot_t(left, right, precision=None):
    return lax.dot_general(
        left, right, (((1,), (1,)), ((), ())),
        preferred_element_type=jnp.float32, precision=precision,
    )


class Sizes:
    def __init__(self, trial_doubles, occ_fock, virt_fock, converged):
        self.local, self.rows, self.pairs = trial_doubles.shape
        self.occ = occ_fock.shape[0]
        self.virt = virt_fock.shape[0]
        self.roots = converged.shape[0]
        self.groups = lax.axis_size("root")
        self.parts = lax.axis_size("virt")
        self.half = self.occ // CORES
        self.per = self.groups // CORES
        self.piece = self.pairs // self.per
        self.slab = self.pairs // self.parts
        self.tiles = self.rows // ROWS
        self.batch = next((g for g in (3, 5, 1) if self.tiles % g == 0))
        self.steps = self.tiles // self.batch
        self.tile = ROWS * self.occ


def fits(trial_doubles, occ_fock, virt_fock, converged):
    s = Sizes(trial_doubles, occ_fock, virt_fock, converged)
    return (
        lax.axis_size("occ") == CORES
        and s.local == CORES
        and s.groups % CORES == 0
        and s.roots == ROWS
        and s.roots == s.local * s.groups
        and s.rows % ROWS == 0
        and s.rows * s.parts == s.virt
        and s.pairs % s.tile == 0
        and s.tile % 128 == 0
        and s.piece % 128 == 0
        and s.slab % 128 == 0
        and s.pairs * CORES == s.occ * s.occ
        and s.occ + s.roots <= 128
    )


def whole_body(
    s, active, singles, trial, flat_trial, occ_fock, virt_fock, ovoo, ooov,
    sigma_out, singles_out, matrix_out,
    sall, mix, unit, second, wide, kron, own, other, slab, product, vv,
    everyone, blocks, kept, sent, got, summed, outer, oo, sigma, sigmas,
    table, square, red0, red1, red2,
    s_one, r_one, s_tri, r_tri, s_fwd, s_own, s_swp, r_swp, s_vin, r_vin, s_vout, r_vout,
    s_blk, s_cor, r_cor, s_out, r_out, s_sig, r_sig, s_res, s_red, r_red,
):
    z, v, c = lax.axis_index("root"), lax.axis_index("virt"), lax.axis_index("occ")
    mate = 1 - c
    groups, parts, per, batch = s.groups, s.parts, s.per, s.batch
    home, place = z // per, z % per
    at_home = home == c

    def turn(index, by, size):
        return lax.rem(index + by, size)

    def remote(src, dst, send, recv, **where):
        return pltpu.make_async_remote_copy(
            src_ref=src, dst_ref=dst, send_sem=send, recv_sem=recv,
            device_id=where, device_id_type=MESH,
        )

    def lanes(index, width):
        return pl.ds(pl.multiple_of(index * width, 128), width)

    def cut(t):
        return pl.ds(t * batch, batch)

    def one_copy(d):
        to = turn(z, d, groups)
        return remote(sall.at[z], sall.at[z], s_one.at[d], r_one.at[z], root=to)

    def one_got(d):
        src = turn(z, d, groups)
        return remote(sall.at[src], sall.at[src], s_one.at[d], r_one.at[src], root=src)

    def trial_copy(j, r):
        to = c * per + j
        core = jnp.where(to == z, mate, r)
        n = z * s.local + r
        return remote(
            trial.at[r, :, :, lanes(j, s.piece)], everyone.at[n],
            s_tri.at[j, r], r_tri.at[n], root=to, occ=core,
        )

    def trial_own(r):
        n = z * s.local + r
        return pltpu.make_async_copy(
            trial.at[r, :, :, lanes(place, s.piece)], everyone.at[n], r_tri.at[n]
        )

    def trial_pass(d):
        n = turn(z, d, groups) * s.local + c
        return remote(everyone.at[n], everyone.at[n], s_fwd.at[d], r_tri.at[n], occ=mate)

    def trial_got(n):
        return remote(everyone.at[n], everyone.at[n], s_fwd.at[0], r_tri.at[n], occ=mate)

    def swap_copy():
        return remote(flat_trial, other, s_swp, r_swp, occ=mate)

    def slab_rows(u):
        return pl.ds(u * s.tiles, s.tiles)

    def slab_copy(d, r):
        u = turn(v, d, parts)
        return remote(
            trial.at[r, :, :, lanes(u, s.slab)], slab.at[r, slab_rows(v)],
            s_vin.at[d, r], r_vin.at[v, r], virt=u,
        )

    def slab_own(r):
        return pltpu.make_async_copy(
            trial.at[r, :, :, lanes(v, s.slab)], slab.at[r, slab_rows(v)], r_vin.at[v, r]
        )

    def slab_got(d, r):
        u = turn(v, d, parts)
        return remote(
            slab.at[r, slab_rows(u)], slab.at[r, slab_rows(u)],
            s_vin.at[d, r], r_vin.at[u, r], virt=u,
        )

    def back_copy(d, r):
        u = turn(v, d, parts)
        return remote(
            product.at[d, r], vv.at[r, :, :, lanes(v, s.slab)],
            s_vout.at[d, r], r_vout.at[v, r], virt=u,
        )

    def back_got(d, r):
        u = turn(v, d, parts)
        return remote(
            product.at[d, r], vv.at[r, :, :, lanes(u, s.slab)],
            s_vout.at[d, r], r_vout.at[u, r], virt=u,
        )

    def load(source, t, slot):
        return pltpu.make_async_copy(
            source.at[:, cut(t)], blocks.at[slot], s_blk.at[slot]
        )

    def core_copy(t):
        return remote(
            sent.at[:, cut(t)], got.at[:, cut(t)], s_cor.at[t], r_cor.at[t], occ=mate
        )

    def outer_copy(t, d):
        to = turn(z, d, groups)
        return remote(
            summed.at[to, cut(t)], outer.at[c, cut(t), :, lanes(place, s.piece)],
            s_out.at[t, d], r_out.at[t, place, c], root=to, occ=home,
        )

    def outer_got(t, j, r):
        src = c * per + j
        core = jnp.where(src == z, mate, r)
        spot = outer.at[r, cut(t), :, lanes(j, s.piece)]
        return remote(spot, spot, s_out.at[t, 0], r_out.at[t, j, r], root=src, occ=core)

    def sigma_copy(t, r, j):
        to = c * per + j
        return remote(
            sigma.at[r, cut(t), :, lanes(j, s.piece)], sigmas.at[z, cut(t)],
            s_sig.at[t, r, j], r_sig.at[t, z], root=to, occ=r,
        )

    def sigma_got(t, d):
        src = turn(z, d, groups)
        core = jnp.where(src == z, mate, home)
        return remote(
            sigmas.at[src, cut(t)], sigmas.at[src, cut(t)],
            s_sig.at[t, 0, 0], r_sig.at[t, src], root=src, occ=core,
        )

    def result_copy(t, r):
        return pltpu.make_async_copy(
            sigma.at[r, cut(t)], sigma_out.at[r, cut(t)], s_res.at[t, r]
        )

    barrier = pltpu.get_barrier_semaphore()
    greeted = 0
    for d in range(groups):
        for e in range(CORES):
            if d or e:
                pl.semaphore_signal(
                    barrier, inc=1, device_id_type=MESH,
                    device_id={"root": turn(z, d, groups), "occ": turn(c, e, CORES)},
                )
                greeted += 1
    for d in range(1, parts):
        pl.semaphore_signal(
            barrier, inc=1, device_id_type=MESH, device_id={"virt": turn(v, d, parts)}
        )
        greeted += 1
    load(ovoo, 0, 0).start()
    row = iota((ROWS, 128), 0)
    mine = jnp.zeros((ROWS, 128), jnp.float32)
    wide_ones = jnp.concatenate(
        [singles[...].astype(jnp.float32), jnp.zeros((s.local, 128 - s.occ), jnp.float32)], axis=1
    )
    for r in range(s.local):
        mine = jnp.where(row == z * s.local + r, wide_ones[r : r + 1, :], mine)
    sall[z] = mine
    pl.semaphore_wait(barrier, greeted)

    for d in range(1, groups):
        one_copy(d).start()
    for j in range(per):
        for r in range(s.local):
            trial_copy(j, r).start()

    @pl.when(at_home)
    def _():
        for r in range(s.local):
            trial_own(r).start()

    for r in range(s.local):
        for d in range(1, parts):
            slab_copy(d, r).start()
        slab_own(r).start()
    swap_copy().start()
    own_copy = pltpu.make_async_copy(flat_trial, own, s_own)
    own_copy.start()

    line = iota((s.occ, s.tile), 0)
    lane = iota((s.occ, s.tile), 1)
    spots = line == lane
    for i in range(1, ROWS):
        spots = spots | (line + i * s.occ == lane)
    unit[...] = one_hot(spots)
    spread_fock = dot(occ_fock[...], unit[...].astype(jnp.bfloat16))
    for i in range(ROWS):
        inside = (lane >= i * s.occ) & (lane < (i + 1) * s.occ)
        second[i * s.occ : (i + 1) * s.occ, :] = jnp.where(inside, spread_fock, 0.0).astype(
            jnp.bfloat16
        )

    def widen(col, carry):
        first = (line - c * s.half) * s.occ - col * s.tile
        pick = (lane >= first) & (lane < first + s.occ)
        wide[:, lanes(col, s.tile)] = dot(occ_fock[...], one_hot(pick, jnp.bfloat16))
        return carry

    columns = s.pairs // s.tile
    lax.fori_loop(0, columns, widen, 0)

    for d in range(1, groups):
        one_got(d).wait_recv()
    everyones = sall[0]
    for g in range(1, groups):
        everyones = everyones + sall[g]
    left = iota((s.roots * ROWS, s.roots), 0) // ROWS
    chosen = jnp.where(
        left < groups, s.local * left + c, s.local * (left - groups) + mate
    )
    left = one_hot(iota((s.roots * ROWS, s.roots), 1) == chosen, jnp.bfloat16)
    right = iota((128, s.half * ROWS), 1) // ROWS + c * s.half
    right = one_hot(iota((128, s.half * ROWS), 0) == right, jnp.bfloat16)
    shape = (s.roots * ROWS, s.half * ROWS)
    mixed = dot(dot(left, everyones.astype(jnp.bfloat16)).astype(jnp.bfloat16), right)
    same = iota(shape, 0) % ROWS == iota(shape, 1) % ROWS
    mix[...] = jnp.where(same, -mixed, 0.0).astype(jnp.bfloat16)

    def finish(t):
        core_copy(t).wait_recv()
        slot = lax.rem(t, 2)
        for g in range(batch):
            tile = t * batch + g
            summed[:, tile] = (kept[slot, :, g] + got[:, tile].astype(jnp.float32)).astype(
                jnp.bfloat16
            )
        for d in range(1, groups):
            outer_copy(t, d).start()

        @pl.when(at_home)
        def _():
            for g in range(batch):
                tile = t * batch + g
                outer[c, tile, :, lanes(place, s.piece)] = summed[z, tile]

        @pl.when(jnp.logical_not(at_home))
        def _():
            outer_copy(t, 0).start()

    def outer_step(t, carry):
        slot = lax.rem(t, 2)

        @pl.when(t + 1 < s.steps)
        def _():
            load(ovoo, t + 1, 1 - slot).start()

        load(ovoo, t, slot).wait()
        for g in range(batch):
            value = dot(mix[...], flat(blocks[slot, :, g]))
            value = value.reshape(s.roots, ROWS, s.piece)
            kept[slot, :, g] = value[:groups]
            sent[:, t * batch + g] = value[groups:].astype(jnp.bfloat16)
        core_copy(t).start()

        @pl.when(t > 0)
        def _():
            finish(t - 1)

        return carry

    lax.fori_loop(0, s.steps, outer_step, 0)
    finish(s.steps - 1)
    load(ooov, 0, 0).start()

    own_copy.wait()
    swap_copy().wait_recv()

    def spread(half, k, here):
        start = pl.multiple_of(half * s.half + k * ROWS, ROWS)
        rows = wide[pl.ds(start, ROWS), here]
        for i in range(ROWS):
            kron[i * s.occ : (i + 1) * s.occ, :] = (unit[...] * rows[i : i + 1, :]).astype(
                jnp.bfloat16
            )

    def column(col, carry):
        here = lanes(col, s.tile)
        oo[:, here] = dot(own[:, here], second[...])

        def inner(k, carry):
            there = lanes(k, s.tile)
            spread(c, k, here)
            oo[:, here] += dot(own[:, there], kron[...])
            spread(mate, k, here)
            oo[:, here] += dot(other[:, there], kron[...])
            return carry

        return lax.fori_loop(0, columns, inner, carry)

    early = columns // 3
    lax.fori_loop(0, early, column, 0)
    for r in range(s.local):
        for d in range(1, parts):
            slab_got(d, r).wait_recv()
        slab_own(r).wait()
    for r in range(s.local):
        amps = flat(slab[r])
        for d in range(1, parts):
            part = dot(virt_fock[turn(v, d, parts)], amps)
            product[d, r] = part.reshape(s.tiles, ROWS, s.slab).astype(jnp.bfloat16)
            back_copy(d, r).start()
        part = dot(virt_fock[v], amps).reshape(s.tiles, ROWS, s.slab)
        vv[r, :, :, lanes(v, s.slab)] = part.astype(jnp.bfloat16)
    lax.fori_loop(early, columns, column, 0)

    for d in range(1, groups):
        trial_got(turn(z, d, groups) * s.local + c).wait_recv()
        trial_pass(d).start()
    for r in range(s.local):
        for d in range(1, parts):
            back_got(d, r).wait_recv()

    def sigma_step(t, carry):
        for r in range(s.local):
            for j in range(per):
                @pl.when(jnp.logical_not((c * per + j == z) & (c == r)))
                def _():
                    outer_got(t, j, r).wait_recv()

            for g in range(batch):
                tile = t * batch + g
                rows = pl.ds(pl.multiple_of(r * s.rows + tile * ROWS, ROWS), ROWS)
                value = (
                    vv[r, tile].astype(jnp.float32)
                    + outer[r, tile].astype(jnp.float32)
                    - oo[rows, :]
                )
                sigma[r, tile] = (active[z * s.local + r] * value).astype(jnp.bfloat16)
            result_copy(t, r).start()
            for j in range(per):
                here = (c * per + j == z) & (c == r)

                @pl.when(jnp.logical_not(here))
                def _():
                    sigma_copy(t, r, j).start()

                @pl.when(here)
                def _():
                    for g in range(batch):
                        tile = t * batch + g
                        sigmas[z, tile] = sigma[r, tile, :, j * s.piece : (j + 1) * s.piece]

        return carry

    lax.fori_loop(0, s.steps, sigma_step, 0)

    for d in range(1, groups):
        trial_got(turn(z, d, groups) * s.local + mate).wait_recv()
    for r in range(s.local):
        trial_got(z * s.local + r).wait_recv()
    table[...] = jnp.zeros_like(table)
    square[...] = jnp.zeros_like(square)

    def coupling_step(t, carry):
        slot = lax.rem(t, 2)

        @pl.when(t + 1 < s.steps)
        def _():
            load(ooov, t + 1, 1 - slot).start()

        load(ooov, t, slot).wait()
        for g in range(batch):
            table[...] += dot_t(flat(everyone[:, t * batch + g]), flat(blocks[slot, :, g]))
        return carry

    lax.fori_loop(0, s.steps, coupling_step, 0)

    def project_step(t, carry):
        for d in range(groups):
            if d:
                sigma_got(t, d).wait_recv()
            else:
                @pl.when(jnp.logical_not(at_home))
                def _():
                    sigma_got(t, 0).wait_recv()

        for g in range(batch):
            tile = t * batch + g
            square[...] += dot_t(flat(everyone[:, tile]), flat(sigmas[:, tile]))
        return carry

    lax.fori_loop(0, s.steps, project_step, 0)

    gather = one_hot(iota((s.roots, s.roots * ROWS), 1) // ROWS == iota((s.roots, s.roots * ROWS), 0))

    def same_row(values, target):
        rows = iota(values.shape, 0) % ROWS == iota(values.shape, 1) % ROWS
        folded = dot(gather, jnp.where(rows, values, 0.0), HIGH)
        width = values.shape[1]
        to = target(iota((width, 128), 0) // ROWS)
        return dot(folded, one_hot(iota((width, 128), 1) == to), HIGH)

    part = same_row(table[...], lambda k: c * s.half + k)
    part = part + same_row(square[...], lambda o: s.occ + s.local * o + c)

    def summed_over(held, index, size, base, name):
        def copy(d):
            return remote(
                held.at[index], held.at[index], s_red.at[base + d], r_red.at[base + index],
                **{name: turn(index, d, size)},
            )

        def got_from(d):
            src = turn(index, d, size)
            return remote(
                held.at[src], held.at[src], s_red.at[base + d], r_red.at[base + src],
                **{name: src},
            )

        for d in range(1, size):
            copy(d).start()
        for d in range(1, size):
            got_from(d).wait_recv()
        total = held[0]
        for g in range(1, size):
            total = total + held[g]
        return total, copy

    red0[c] = part
    total, copy0 = summed_over(red0, c, CORES, 0, "occ")
    red1[v] = total
    total, copy1 = summed_over(red1, v, parts, CORES, "virt")
    red2[z] = total
    total, copy2 = summed_over(red2, z, groups, CORES + parts, "root")

    coupling = total[:, : s.occ]
    ones = everyones[:, : s.occ]
    weight = jnp.zeros((s.roots, 1), jnp.float32)
    for n in range(s.roots):
        weight = jnp.where(iota((s.roots, 1), 0) == n, active[n], weight)
    every = weight * (-dot(ones.astype(jnp.bfloat16), occ_fock[...]) - 0.5 * coupling)
    whole = total[:, s.occ : s.occ + s.roots] / math.sqrt(s.occ * s.occ * s.virt)
    whole = whole + dot_t(ones, every, HIGH) / math.sqrt(s.occ)
    pick = one_hot(
        iota((s.local, s.roots), 1) == iota((s.local, s.roots), 0) + z * s.local
    )
    singles_out[...] = dot(pick, every, HIGH)
    matrix_out[...] = dot(pick, whole, HIGH)

    for d in range(1, groups):
        one_copy(d).wait_send()
        trial_pass(d).wait_send()
        copy2(d).wait_send()
    for d in range(1, parts):
        copy1(d).wait_send()
        for r in range(s.local):
            slab_copy(d, r).wait_send()
            back_copy(d, r).wait_send()
    copy0(1).wait_send()
    swap_copy().wait_send()
    for j in range(per):
        for r in range(s.local):
            trial_copy(j, r).wait_send()

    def drain(t, carry):
        core_copy(t).wait_send()
        for d in range(1, groups):
            outer_copy(t, d).wait_send()

        @pl.when(jnp.logical_not(at_home))
        def _():
            outer_copy(t, 0).wait_send()

        for r in range(s.local):
            result_copy(t, r).wait()
            for j in range(per):
                @pl.when(jnp.logical_not((c * per + j == z) & (c == r)))
                def _():
                    sigma_copy(t, r, j).wait_send()

        return carry

    lax.fori_loop(0, s.steps, drain, 0)


def local(trial_singles, trial_doubles, occ_fock, virt_fock, w_ovoo, w_ooov, converged):
    if not fits(trial_doubles, occ_fock, virt_fock, converged):
        return plain(trial_singles, trial_doubles, occ_fock, virt_fock, w_ovoo, w_ooov, converged)
    s = Sizes(trial_doubles, occ_fock, virt_fock, converged)
    active = (1 - converged).astype(jnp.float32)
    trial = trial_doubles.reshape(s.local, s.tiles, ROWS, s.pairs)
    flat_trial = trial_doubles.reshape(s.local * s.rows, s.pairs)
    fock = virt_fock.reshape(s.parts, s.rows, s.virt)
    outer_in = w_ovoo.reshape(s.half, s.tiles, ROWS, s.piece)
    coupling_in = w_ooov.reshape(s.half, s.tiles, ROWS, s.piece)
    bf, f32 = jnp.bfloat16, jnp.float32
    anywhere = pl.BlockSpec(memory_space=pl.ANY)
    vmem = pl.BlockSpec(memory_space=pltpu.VMEM)
    smem = pl.BlockSpec(memory_space=pltpu.SMEM)
    dma, n = pltpu.SemaphoreType.DMA, s.roots * ROWS
    wide_tile = (s.tiles, ROWS, s.piece)
    sigma, singles, matrix = pl.pallas_call(
        functools.partial(whole_body, s),
        in_specs=[smem, vmem, anywhere, anywhere, vmem, vmem, anywhere, anywhere],
        out_specs=[anywhere, vmem, vmem],
        out_shape=[
            jax.ShapeDtypeStruct(trial.shape, bf),
            jax.ShapeDtypeStruct((s.local, s.occ), f32),
            jax.ShapeDtypeStruct((s.local, s.roots), f32),
        ],
        scratch_shapes=[
            pltpu.VMEM((s.groups, ROWS, 128), f32),
            pltpu.VMEM((n, s.half * ROWS), bf),
            pltpu.VMEM((s.occ, s.tile), f32),
            pltpu.VMEM((s.tile, s.tile), bf),
            pltpu.VMEM((s.occ, s.pairs), f32),
            pltpu.VMEM((s.tile, s.tile), bf),
            pltpu.VMEM(flat_trial.shape, bf),
            pltpu.VMEM(flat_trial.shape, bf),
            pltpu.VMEM((s.local, s.parts * s.tiles, ROWS, s.slab), bf),
            pltpu.VMEM((s.parts, s.local, s.tiles, ROWS, s.slab), bf),
            pltpu.VMEM(trial.shape, bf),
            pltpu.VMEM((s.roots,) + wide_tile, bf),
            pltpu.VMEM((2, s.half, s.batch, ROWS, s.piece), bf),
            pltpu.VMEM((2, s.groups, s.batch, ROWS, s.piece), f32),
            pltpu.VMEM((s.groups,) + wide_tile, bf),
            pltpu.VMEM((s.groups,) + wide_tile, bf),
            pltpu.VMEM((s.groups,) + wide_tile, bf),
            pltpu.VMEM(trial.shape, bf),
            pltpu.VMEM(flat_trial.shape, f32),
            pltpu.VMEM(trial.shape, bf),
            pltpu.VMEM((s.groups,) + wide_tile, bf),
            pltpu.VMEM((n, s.half * ROWS), f32),
            pltpu.VMEM((n, s.groups * ROWS), f32),
            pltpu.VMEM((CORES, ROWS, 128), f32),
            pltpu.VMEM((s.parts, ROWS, 128), f32),
            pltpu.VMEM((s.groups, ROWS, 128), f32),
            dma((s.groups,)), dma((s.groups,)),
            dma((s.per, s.local)), dma((s.roots,)), dma((s.groups,)), dma(()),
            dma(()), dma(()),
            dma((s.parts, s.local)), dma((s.parts, s.local)),
            dma((s.parts, s.local)), dma((s.parts, s.local)),
            dma((2,)), dma((s.steps,)), dma((s.steps,)),
            dma((s.steps, s.groups)), dma((s.steps, s.per, s.local)),
            dma((s.steps, s.local, s.per)), dma((s.steps, s.groups)),
            dma((s.steps, s.local)),
            dma((CORES + s.parts + s.groups,)), dma((CORES + s.parts + s.groups,)),
        ],
        compiler_params=pltpu.CompilerParams(
            collective_id=0, has_side_effects=True, vmem_limit_bytes=66 * 1000 * 1000
        ),
        cost_estimate=pl.CostEstimate(
            flops=8 * s.rows * s.pairs * s.pairs, bytes_accessed=4 * w_ovoo.size, transcendentals=0
        ),
        name="sigma_step",
    )(active, trial_singles, trial, flat_trial, occ_fock, fock, outer_in, coupling_in)
    return (sigma.reshape(trial_doubles.shape), singles, matrix)


def solution(mesh):
    placed = (
        P("root", None),
        P("root", "virt", "occ"),
        P(),
        P(),
        P("occ", "virt", "root"),
        P("occ", "virt", "root"),
        P(),
    )
    return jax.shard_map(
        local,
        mesh=mesh,
        in_specs=placed,
        out_specs=(P("root", "virt", "occ"), P("root", None), P("root", None)),
        check_vma=False,
    )
```

```python
import functools
import math

import jax
import jax.numpy as jnp
from jax import lax
from jax.experimental import pallas as pl
from jax.experimental.pallas import tpu as pltpu
from jax.sharding import PartitionSpec as P


def flat_pairs(left, right):
    return lax.dot_general(
        left.reshape(left.shape[0], -1),
        right.reshape(right.shape[0], -1),
        (((1,), (1,)), ((), ())),
        preferred_element_type=jnp.float32,
    )


def plain(trial_singles, trial_doubles, occ_fock, virt_fock, w_ovoo, w_ooov, converged):
    local_roots, virt_local, pair_local = trial_doubles.shape
    occ_count = occ_fock.shape[0]
    virt_count = virt_fock.shape[0]
    root_count = converged.shape[0]
    root_groups = lax.axis_size("root")
    occ_groups = lax.axis_size("occ")
    root_index = lax.axis_index("root")
    occ_index = lax.axis_index("occ")
    occ_half = occ_count // occ_groups
    block_pairs = occ_count * occ_count // root_groups
    own_start = occ_index * occ_half
    active = (1 - converged).astype(jnp.float32)
    own_active = lax.dynamic_slice_in_dim(active, root_index * local_roots, local_roots)
    singles_all = lax.all_gather(trial_singles, "root", axis=0, tiled=True)
    gathered = lax.all_gather(trial_doubles, "occ", axis=2, tiled=True)
    fock_cols = lax.dynamic_slice_in_dim(occ_fock, own_start, occ_half, 1)
    batch_rows = local_roots * virt_local
    stacked = gathered.reshape(batch_rows, occ_count, occ_count)
    first_term = jnp.einsum(
        "ki,bkj->bij", fock_cols, stacked, preferred_element_type=jnp.float32
    ).reshape(local_roots, virt_local, pair_local)
    own_rows = trial_doubles.reshape(batch_rows, occ_half, occ_count)
    second_term = jnp.einsum(
        "bik,kj->bij", own_rows, occ_fock, preferred_element_type=jnp.float32
    ).reshape(local_roots, virt_local, pair_local)
    doubles_block = lax.all_to_all(gathered, "root", split_axis=2, concat_axis=0, tiled=True)
    partial_coupling = flat_pairs(doubles_block, w_ooov)
    coupling_part = lax.dynamic_update_slice(
        jnp.zeros((root_count, occ_count), jnp.float32), partial_coupling, (jnp.int32(0), own_start)
    )
    coupling = lax.psum(coupling_part, ("root", "virt", "occ"))
    singles_fock = jnp.dot(singles_all, occ_fock, preferred_element_type=jnp.float32)
    singles_every = active[:, None] * (-singles_fock - 0.5 * coupling)
    sigma_singles = lax.dynamic_slice_in_dim(singles_every, root_index * local_roots, local_roots)
    singles_cols = lax.dynamic_slice_in_dim(singles_all, own_start, occ_half, 1)
    outer_part = (
        -jnp.dot(singles_cols, w_ovoo.reshape(occ_half, -1), preferred_element_type=jnp.float32)
    ).reshape(root_count, virt_local, block_pairs)
    product = jnp.einsum(
        "ac,ncp->nap",
        virt_fock,
        lax.all_to_all(trial_doubles, "virt", split_axis=2, concat_axis=1, tiled=True),
        preferred_element_type=jnp.float32,
    ).astype(jnp.bfloat16)
    vv_term = lax.all_to_all(product, "virt", split_axis=1, concat_axis=2, tiled=True)
    vv_value = vv_term.astype(jnp.float32)
    outer_own = lax.all_to_all(outer_part, "root", split_axis=0, concat_axis=2, tiled=True)
    outer_half = lax.psum_scatter(outer_own, "occ", scatter_dimension=2, tiled=True)
    summed = vv_value + outer_half - first_term - second_term
    sigma_doubles = (own_active[:, None, None] * summed).astype(jnp.bfloat16)
    trial_piece, sigma_piece = (
        lax.all_to_all(trial_doubles, "root", split_axis=2, concat_axis=0, tiled=True),
        lax.all_to_all(sigma_doubles, "root", split_axis=2, concat_axis=0, tiled=True),
    )
    doubles_part = lax.psum(flat_pairs(trial_piece, sigma_piece), ("root", "virt", "occ"))
    singles_part = jnp.dot(
        singles_all.astype(jnp.float32), singles_every.T, precision=lax.Precision.HIGHEST
    )
    whole_matrix = doubles_part / math.sqrt(
        occ_count * occ_count * virt_count
    ) + singles_part / math.sqrt(occ_count)
    subspace = lax.dynamic_slice_in_dim(whole_matrix, root_index * local_roots, local_roots, 0)
    return (sigma_doubles, sigma_singles, subspace)


ROWS = 8
MESH = pl.DeviceIdType.MESH
HIGH = lax.Precision.HIGHEST
CORES = 2


def flat(block):
    count, rows, width = block.shape
    return block.astype(jnp.float32).reshape(count * rows, width).astype(jnp.bfloat16)


def iota(shape, axis):
    return lax.broadcasted_iota(jnp.int32, shape, axis)


def one_hot(mask, dtype=jnp.float32):
    return jnp.where(mask, 1.0, 0.0).astype(dtype)


def dot(left, right, precision=None):
    return jnp.dot(left, right, preferred_element_type=jnp.float32, precision=precision)


def dot_t(left, right, precision=None):
    return lax.dot_general(
        left, right, (((1,), (1,)), ((), ())),
        preferred_element_type=jnp.float32, precision=precision,
    )


class Sizes:
    def __init__(self, trial_doubles, occ_fock, virt_fock, converged):
        self.local, self.rows, self.pairs = trial_doubles.shape
        self.occ = occ_fock.shape[0]
        self.virt = virt_fock.shape[0]
        self.roots = converged.shape[0]
        self.groups = lax.axis_size("root")
        self.parts = lax.axis_size("virt")
        self.half = self.occ // CORES
        self.per = self.groups // CORES
        self.piece = self.pairs // self.per
        self.slots = self.roots // 2
        self.tiles = self.rows // ROWS
        self.batch = next((g for g in (3, 5, 1) if self.tiles % g == 0))
        self.steps = self.tiles // self.batch
        self.tile = ROWS * self.occ
        self.thirds = self.piece // self.tile
        self.slab = self.tile // CORES


def fits(trial_doubles, occ_fock, virt_fock, converged):
    s = Sizes(trial_doubles, occ_fock, virt_fock, converged)
    return (
        lax.axis_size("occ") == CORES
        and s.local == CORES
        and s.groups == 4
        and s.parts == 4
        and s.roots == ROWS
        and s.roots == s.local * s.groups
        and s.rows % ROWS == 0
        and s.rows * s.parts == s.virt
        and s.piece % s.tile == 0
        and s.slab % 128 == 0
        and s.pairs * CORES == s.occ * s.occ
        and s.occ + s.roots <= 128
    )


def whole_body(
    s, converged, singles, trial, flat_trial, occ_fock, virt_fock, ovoo, ooov,
    sigma_out, singles_out, matrix_out,
    sall, mix, unit, second, wide, kron, own, other, slab, product, vv,
    everyone, blocks, kept, sent, got, summed, oo, sigma,
    rest, near, across, far, handed, taken,
    table, square, red0, red1, red2,
    s_one, r_one, s_tri, r_tri, s_fwd, s_own, s_swp, r_swp, s_vin, r_vin, s_vout, r_vout,
    s_blk, s_cor, r_cor, s_near, r_near, s_far, r_far, s_pass, r_pass, s_hand, r_hand,
    s_res, s_red, r_red,
):
    z, v, c = lax.axis_index("root"), lax.axis_index("virt"), lax.axis_index("occ")
    mate = 1 - c
    groups, parts, per, batch = s.groups, s.parts, s.per, s.batch
    home, place = z // per, z % per
    at_home = home == c
    beside = home * per + 1 - place
    opposite = lax.rem(z + per, groups)

    slot_of, count = [], jnp.int32(0)
    for n in range(s.roots):
        live = 1 - converged[n]
        slot_of.append(jnp.where(live == 1, count, -1))
        count = count + live

    def slots_at(group):
        found = []
        for r in range(s.local):
            value = slot_of[r]
            for g in range(1, groups):
                value = jnp.where(group == g, slot_of[g * s.local + r], value)
            found.append(value)
        return found

    my_slots, near_slots = slots_at(z), slots_at(beside)
    weights = [jnp.where(value >= 0, 1.0, 0.0) for value in my_slots]

    def choose(number, values):
        result = values[0]
        for k in range(1, len(values)):
            result = lax.select(number == k, values[k], result)
        return result

    def of_half(k, inside, beyond):
        value = beyond
        for r in range(s.local):
            value = lax.select(my_slots[r] == k, inside[r], value)
            value = lax.select(near_slots[r] == k, inside[s.local + r], value)
        return value

    def turn(index, by, size):
        return lax.rem(index + by, size)

    def remote(src, dst, send, recv, **where):
        return pltpu.make_async_remote_copy(
            src_ref=src, dst_ref=dst, send_sem=send, recv_sem=recv,
            device_id=where, device_id_type=MESH,
        )

    def lanes(index, width):
        return pl.ds(pl.multiple_of(index * width, 128), width)

    def cut(t):
        return pl.ds(t * batch, batch)

    def one_copy(d):
        to = turn(z, d, groups)
        return remote(sall.at[z], sall.at[z], s_one.at[d], r_one.at[z], root=to)

    def one_got(d):
        src = turn(z, d, groups)
        return remote(sall.at[src], sall.at[src], s_one.at[d], r_one.at[src], root=src)

    def trial_copy(j, r):
        to = c * per + j
        core = jnp.where(to == z, mate, r)
        n = z * s.local + r
        return remote(
            trial.at[r, :, :, lanes(j, s.piece)], everyone.at[n],
            s_tri.at[j, r], r_tri.at[n], root=to, occ=core,
        )

    def trial_own(r):
        n = z * s.local + r
        return pltpu.make_async_copy(
            trial.at[r, :, :, lanes(place, s.piece)], everyone.at[n], r_tri.at[n]
        )

    def trial_pass(d):
        n = turn(z, d, groups) * s.local + c
        return remote(everyone.at[n], everyone.at[n], s_fwd.at[d], r_tri.at[n], occ=mate)

    def trial_got(n):
        return remote(everyone.at[n], everyone.at[n], s_fwd.at[0], r_tri.at[n], occ=mate)

    def swap_copy():
        return remote(flat_trial, other, s_swp, r_swp, occ=mate)

    def slab_rows(u):
        return pl.ds(u * s.tiles, s.tiles)

    def share(u, i):
        start = (u // CORES) * s.piece + i * s.tile + lax.rem(u, CORES) * s.slab
        return pl.ds(pl.multiple_of(start, 128), s.slab)

    def slab_copy(i, d, r):
        u = turn(v, d, parts)
        return remote(
            trial.at[r, :, :, share(u, i)], slab.at[i, r, slab_rows(v)],
            s_vin.at[i, d, r], r_vin.at[i, v, r], virt=u,
        )

    def slab_own(i, r):
        return pltpu.make_async_copy(
            trial.at[r, :, :, share(v, i)], slab.at[i, r, slab_rows(v)], r_vin.at[i, v, r]
        )

    def slab_got(i, d, r):
        u = turn(v, d, parts)
        spot = slab.at[i, r, slab_rows(u)]
        return remote(spot, spot, s_vin.at[i, d, r], r_vin.at[i, u, r], virt=u)

    def back_copy(i, d):
        return remote(
            product.at[i, d - 1], vv.at[v, i],
            s_vout.at[i, d], r_vout.at[i, v], virt=turn(v, d, parts),
        )

    def back_got(i, d):
        u = turn(v, d, parts)
        return remote(
            product.at[i, d - 1], vv.at[u, i], s_vout.at[i, d], r_vout.at[i, u], virt=u
        )

    def vv_at(r, tile, j, i):
        parts_of = [vv[j * CORES + h, i, r, tile] for h in range(CORES)]
        return jnp.concatenate([p.astype(jnp.float32) for p in parts_of], axis=1)

    def load(source, t, slot):
        return pltpu.make_async_copy(
            source.at[:, cut(t)], blocks.at[slot], s_blk.at[slot]
        )

    def core_copy(t):
        return remote(
            sent.at[:, cut(t)], got.at[:, cut(t)], s_cor.at[t], r_cor.at[t], occ=mate
        )

    def third(i, quarter=0):
        return lanes(quarter * s.thirds + i, s.tile)

    def near_copy(i):
        return remote(
            rest.at[(1 - place) * s.thirds + i], near.at[i],
            s_near.at[i], r_near.at[i], root=beside,
        )

    def far_copy(i):
        return remote(across.at[i], far.at[i], s_far.at[i], r_far.at[i], root=opposite)

    def pass_copy(i):
        return remote(far.at[i], far.at[i], s_pass.at[i], r_pass.at[i], occ=mate)

    def hand_copy(i):
        return remote(handed.at[i], taken.at[i], s_hand.at[i], r_hand.at[i], root=beside)

    def result_copy(i, r, j):
        here = third(i, j)
        return pltpu.make_async_copy(
            sigma.at[r, :, :, here], sigma_out.at[r, :, :, here], s_res.at[i, r, j]
        )

    barrier = pltpu.get_barrier_semaphore()
    greeted = 0
    for d in range(groups):
        for e in range(CORES):
            if d or e:
                pl.semaphore_signal(
                    barrier, inc=1, device_id_type=MESH,
                    device_id={"root": turn(z, d, groups), "occ": turn(c, e, CORES)},
                )
                greeted += 1
    for d in range(1, parts):
        pl.semaphore_signal(
            barrier, inc=1, device_id_type=MESH, device_id={"virt": turn(v, d, parts)}
        )
        greeted += 1
    load(ovoo, 0, 0).start()
    row = iota((ROWS, 128), 0)
    mine = jnp.zeros((ROWS, 128), jnp.float32)
    wide_ones = jnp.concatenate(
        [singles[...].astype(jnp.float32), jnp.zeros((s.local, 128 - s.occ), jnp.float32)], axis=1
    )
    for r in range(s.local):
        mine = jnp.where(row == z * s.local + r, wide_ones[r : r + 1, :], mine)
    sall[z] = mine
    pl.semaphore_wait(barrier, greeted)

    for d in range(1, groups):
        one_copy(d).start()
    for j in range(per):
        for r in range(s.local):
            trial_copy(j, r).start()

    @pl.when(at_home)
    def _():
        for r in range(s.local):
            trial_own(r).start()

    def slab_start(i):
        for r in range(s.local):
            for d in range(1, parts):
                slab_copy(i, d, r).start()
            slab_own(i, r).start()

    for i in range(s.thirds - 1):
        slab_start(i)
    swap_copy().start()
    own_copy = pltpu.make_async_copy(flat_trial, own, s_own)
    own_copy.start()

    line = iota((s.occ, s.tile), 0)
    lane = iota((s.occ, s.tile), 1)
    spots = line == lane
    for i in range(1, ROWS):
        spots = spots | (line + i * s.occ == lane)
    unit[...] = one_hot(spots)
    spread_fock = dot(occ_fock[...], unit[...].astype(jnp.bfloat16))
    for i in range(ROWS):
        inside = (lane >= i * s.occ) & (lane < (i + 1) * s.occ)
        second[i * s.occ : (i + 1) * s.occ, :] = jnp.where(inside, spread_fock, 0.0).astype(
            jnp.bfloat16
        )

    def widen(col, carry):
        first = (line - c * s.half) * s.occ - col * s.tile
        pick = (lane >= first) & (lane < first + s.occ)
        wide[:, lanes(col, s.tile)] = dot(occ_fock[...], one_hot(pick, jnp.bfloat16))
        return carry

    columns = s.pairs // s.tile
    lax.fori_loop(0, columns, widen, 0)

    for d in range(1, groups):
        one_got(d).wait_recv()
    everyones = sall[0]
    for g in range(1, groups):
        everyones = everyones + sall[g]
    shape = (s.slots * ROWS, s.roots)
    left = iota(shape, 0) < 0
    for n in range(s.roots):
        left = left | ((iota(shape, 0) // ROWS == slot_of[n]) & (iota(shape, 1) == n))
    left = one_hot(left, jnp.bfloat16)
    right = iota((128, s.half * ROWS), 1) // ROWS + c * s.half
    right = one_hot(iota((128, s.half * ROWS), 0) == right, jnp.bfloat16)
    shape = (s.slots * ROWS, s.half * ROWS)
    mixed = dot(dot(left, everyones.astype(jnp.bfloat16)).astype(jnp.bfloat16), right)
    same = iota(shape, 0) % ROWS == iota(shape, 1) % ROWS
    mix[...] = jnp.where(same, -mixed, 0.0).astype(jnp.bfloat16)

    def finish(t):
        core_copy(t).wait_recv()
        slot = lax.rem(t, 2)
        for g in range(batch):
            tile = t * batch + g
            summed[:, tile] = (kept[slot, :, g] + got[:, tile].astype(jnp.float32)).astype(
                jnp.bfloat16
            )

    def virtual(i):
        for r in range(s.local):
            for d in range(1, parts):
                slab_got(i, d, r).wait_recv()
            slab_own(i, r).wait()
            amps = flat(slab[i, r])
            for d in range(1, parts):
                part = dot(virt_fock[turn(v, d, parts)], amps)
                product[i, d - 1, r] = part.reshape(s.tiles, ROWS, s.slab).astype(jnp.bfloat16)
            part = dot(virt_fock[v], amps).reshape(s.tiles, ROWS, s.slab)
            vv[v, i, r] = part.astype(jnp.bfloat16)
        for d in range(1, parts):
            back_copy(i, d).start()

    def outer_step(t, carry):
        slot = lax.rem(t, 2)

        @pl.when(t + 1 < s.steps)
        def _():
            load(ovoo, t + 1, 1 - slot).start()

        load(ovoo, t, slot).wait()
        for g in range(batch):
            value = dot(mix[...], flat(blocks[slot, :, g]))
            value = value.reshape(s.slots, ROWS, s.piece)
            kept[slot, :, g] = value
            sent[:, t * batch + g] = value.astype(jnp.bfloat16)
        core_copy(t).start()

        @pl.when(t > 0)
        def _():
            finish(t - 1)

        @pl.when(t == s.steps // 2)
        def _():
            virtual(0)
            slab_start(s.thirds - 1)

        return carry

    lax.fori_loop(0, s.steps, outer_step, 0)
    finish(s.steps - 1)
    load(ooov, 0, 0).start()
    lax.fori_loop(1, s.thirds - 1, lambda i, carry: (virtual(i), carry)[1], 0)

    own_copy.wait()
    swap_copy().wait_recv()

    def spread(half, k, here):
        start = pl.multiple_of(half * s.half + k * ROWS, ROWS)
        rows = wide[pl.ds(start, ROWS), here]
        for i in range(ROWS):
            kron[i * s.occ : (i + 1) * s.occ, :] = (unit[...] * rows[i : i + 1, :]).astype(
                jnp.bfloat16
            )

    def column(col, carry):
        here = lanes(col, s.tile)
        oo[:, here] = dot(own[:, here], second[...])

        def inner(k, carry):
            there = lanes(k, s.tile)
            spread(c, k, here)
            oo[:, here] += dot(own[:, there], kron[...])
            spread(mate, k, here)
            oo[:, here] += dot(other[:, there], kron[...])
            return carry

        return lax.fori_loop(0, columns, inner, carry)

    def each_tile(body):
        def step(tile, carry):
            body(tile)
            return carry

        lax.fori_loop(0, s.tiles, step, 0)

    def rows_of(r, tile):
        return pl.ds(pl.multiple_of(r * s.rows + tile * ROWS, ROWS), ROWS)

    def summed_at(k, tile, i):
        return summed[k, tile, :, third(i)]

    def far_at(k, tile, i):
        return far[i, k, tile]

    def hand(source, i):
        def body(tile):
            values = [source(k, tile, i) for k in range(s.slots)]
            for r in range(s.local):
                handed[i, r, tile] = choose(near_slots[r], values)

        each_tile(body)
        hand_copy(i).start()

    def inside_at(tile, i):
        own_part = [rest[place * s.thirds + i, r, tile] for r in range(s.local)]
        return own_part + [near[i, r, tile] for r in range(s.local)]

    def cross(i):
        near_copy(i).wait_recv()

        @pl.when(at_home)
        def _():
            hand(summed_at, i)

        @pl.when(jnp.logical_not(at_home))
        def _():
            def body(tile):
                inside = inside_at(tile, i)
                for k in range(s.slots):
                    across[i, k, tile] = of_half(k, inside, summed_at(k, tile, i))

            each_tile(body)
            far_copy(i).start()

    def rest_step(i, carry):
        def quarter(j, carry):
            @pl.when((j == 1) & (i > 0))
            def _():
                cross(i - 1)

            @pl.when((j == 1) & (i == 0))
            def _():
                virtual(s.thirds - 1)

            return column(j * s.thirds + i, carry)

        lax.fori_loop(0, per, quarter, 0)
        for d in range(1, parts):
            back_got(i, d).wait_recv()

        def body(tile):
            for r in range(s.local):
                for j in range(per):
                    value = vv_at(r, tile, j, i) - oo[rows_of(r, tile), third(i, j)]
                    rest[j * s.thirds + i, r, tile] = value.astype(jnp.bfloat16)

        each_tile(body)
        near_copy(i).start()
        return carry

    lax.fori_loop(0, s.thirds, rest_step, 0)
    cross(s.thirds - 1)

    table[...] = jnp.zeros_like(table)
    square[...] = jnp.zeros_like(square)

    def coupling_step(t, carry):
        slot = lax.rem(t, 2)

        @pl.when(t + 1 < s.steps)
        def _():
            load(ooov, t + 1, 1 - slot).start()

        load(ooov, t, slot).wait()
        for g in range(batch):
            table[...] += dot_t(flat(everyone[:, t * batch + g]), flat(blocks[slot, :, g]))
        return carry

    def forward(i):
        @pl.when(at_home)
        def _():
            far_copy(i).wait_recv()
            pass_copy(i).start()

        @pl.when(jnp.logical_not(at_home))
        def _():
            pass_copy(i).wait_recv()
            hand(far_at, i)

    def sigma_step(i):
        hand_copy(i).wait_recv()

        def finish_tile(source):
            def body(tile):
                values = [source(k, tile, i) for k in range(s.slots)]
                for r in range(s.local):
                    mine = choose(my_slots[r], values)
                    for j, outer in ((place, mine), (1 - place, taken[i, r, tile])):
                        here = third(i, j)
                        value = (
                            vv_at(r, tile, j, i)
                            + outer.astype(jnp.float32)
                            - oo[rows_of(r, tile), here]
                        )
                        sigma[r, tile, :, here] = (weights[r] * value).astype(jnp.bfloat16)

            each_tile(body)

        @pl.when(at_home)
        def _():
            finish_tile(summed_at)

        @pl.when(jnp.logical_not(at_home))
        def _():
            finish_tile(far_at)

        for r in range(s.local):
            for j in range(per):
                result_copy(i, r, j).start()

    for i in range(s.thirds - 1):
        forward(i)
    for d in range(1, groups):
        trial_got(turn(z, d, groups) * s.local + c).wait_recv()
        trial_pass(d).start()
    for d in range(1, groups):
        trial_got(turn(z, d, groups) * s.local + mate).wait_recv()
    for r in range(s.local):
        trial_got(z * s.local + r).wait_recv()

    lax.fori_loop(0, s.steps, coupling_step, 0)
    forward(s.thirds - 1)

    @pl.when(at_home)
    def _():
        def body(tile):
            for i in range(s.thirds):
                inside = inside_at(tile, i)
                values = [
                    summed_at(k, tile, i).astype(jnp.float32)
                    + of_half(k, inside, far_at(k, tile, i)).astype(jnp.float32)
                    for k in range(s.slots)
                ]
                values = jnp.concatenate(values, axis=0).astype(jnp.bfloat16)
                square[...] += dot_t(flat(everyone[:, tile, :, third(i)]), values)

        each_tile(body)

    gather = one_hot(iota((s.roots, s.roots * ROWS), 1) // ROWS == iota((s.roots, s.roots * ROWS), 0))

    def same_row(values, target):
        rows = iota(values.shape, 0) % ROWS == iota(values.shape, 1) % ROWS
        folded = dot(gather, jnp.where(rows, values, 0.0), HIGH)
        width = values.shape[1]
        to = target(iota((width, 128), 0) // ROWS, iota((width, 128), 1))
        return dot(folded, one_hot(to), HIGH)

    def root_lane(k, lane):
        found = lane < 0
        for n in range(s.roots):
            found = found | ((k == slot_of[n]) & (lane == s.occ + n))
        return found

    part = same_row(table[...], lambda k, lane: lane == c * s.half + k)
    part = part + same_row(square[...], root_lane)

    def summed_over(held, index, size, base, name):
        def copy(d):
            return remote(
                held.at[index], held.at[index], s_red.at[base + d], r_red.at[base + index],
                **{name: turn(index, d, size)},
            )

        def got_from(d):
            src = turn(index, d, size)
            return remote(
                held.at[src], held.at[src], s_red.at[base + d], r_red.at[base + src],
                **{name: src},
            )

        for d in range(1, size):
            copy(d).start()

        def total():
            for d in range(1, size):
                got_from(d).wait_recv()
            value = held[0]
            for g in range(1, size):
                value = value + held[g]
            return value

        return total, copy

    red0[c] = part
    total, copy0 = summed_over(red0, c, CORES, 0, "occ")
    for i in range(s.thirds - 1):
        sigma_step(i)
    red1[v] = total()
    total, copy1 = summed_over(red1, v, parts, CORES, "virt")
    sigma_step(s.thirds - 1)
    red2[z] = total()
    total, copy2 = summed_over(red2, z, groups, CORES + parts, "root")
    total = total()

    coupling = total[:, : s.occ]
    ones = everyones[:, : s.occ]
    weight = jnp.zeros((s.roots, 1), jnp.float32)
    for n in range(s.roots):
        live = jnp.where(slot_of[n] >= 0, 1.0, 0.0)
        weight = jnp.where(iota((s.roots, 1), 0) == n, live, weight)
    every = weight * (-dot(ones.astype(jnp.bfloat16), occ_fock[...]) - 0.5 * coupling)
    whole = total[:, s.occ : s.occ + s.roots] / math.sqrt(s.occ * s.occ * s.virt)
    whole = whole + dot_t(ones, every, HIGH) / math.sqrt(s.occ)
    pick = one_hot(
        iota((s.local, s.roots), 1) == iota((s.local, s.roots), 0) + z * s.local
    )
    singles_out[...] = dot(pick, every, HIGH)
    matrix_out[...] = dot(pick, whole, HIGH)

    for d in range(1, groups):
        one_copy(d).wait_send()
        trial_pass(d).wait_send()
        copy2(d).wait_send()
    for d in range(1, parts):
        copy1(d).wait_send()
    copy0(1).wait_send()
    swap_copy().wait_send()
    for j in range(per):
        for r in range(s.local):
            trial_copy(j, r).wait_send()

    def drain_core(t, carry):
        core_copy(t).wait_send()
        return carry

    lax.fori_loop(0, s.steps, drain_core, 0)

    def drain(i, carry):
        for r in range(s.local):
            for d in range(1, parts):
                slab_copy(i, d, r).wait_send()
            for j in range(per):
                result_copy(i, r, j).wait()
        for d in range(1, parts):
            back_copy(i, d).wait_send()
        near_copy(i).wait_send()
        hand_copy(i).wait_send()

        @pl.when(at_home)
        def _():
            pass_copy(i).wait_send()

        @pl.when(jnp.logical_not(at_home))
        def _():
            far_copy(i).wait_send()

        return carry

    lax.fori_loop(0, s.thirds, drain, 0)


def local(trial_singles, trial_doubles, occ_fock, virt_fock, w_ovoo, w_ooov, converged):
    if not fits(trial_doubles, occ_fock, virt_fock, converged):
        return plain(trial_singles, trial_doubles, occ_fock, virt_fock, w_ovoo, w_ooov, converged)
    s = Sizes(trial_doubles, occ_fock, virt_fock, converged)
    trial = trial_doubles.reshape(s.local, s.tiles, ROWS, s.pairs)
    flat_trial = trial_doubles.reshape(s.local * s.rows, s.pairs)
    fock = virt_fock.reshape(s.parts, s.rows, s.virt)
    outer_in = w_ovoo.reshape(s.half, s.tiles, ROWS, s.piece)
    coupling_in = w_ooov.reshape(s.half, s.tiles, ROWS, s.piece)
    bf, f32 = jnp.bfloat16, jnp.float32
    anywhere = pl.BlockSpec(memory_space=pl.ANY)
    vmem = pl.BlockSpec(memory_space=pltpu.VMEM)
    smem = pl.BlockSpec(memory_space=pltpu.SMEM)
    dma, n = pltpu.SemaphoreType.DMA, s.roots * ROWS
    wide_tile, third_tile = (s.tiles, ROWS, s.piece), (s.tiles, ROWS, s.tile)
    sigma, singles, matrix = pl.pallas_call(
        functools.partial(whole_body, s),
        in_specs=[smem, vmem, anywhere, anywhere, vmem, vmem, anywhere, anywhere],
        out_specs=[anywhere, vmem, vmem],
        out_shape=[
            jax.ShapeDtypeStruct(trial.shape, bf),
            jax.ShapeDtypeStruct((s.local, s.occ), f32),
            jax.ShapeDtypeStruct((s.local, s.roots), f32),
        ],
        scratch_shapes=[
            pltpu.VMEM((s.groups, ROWS, 128), f32),
            pltpu.VMEM((s.slots * ROWS, s.half * ROWS), bf),
            pltpu.VMEM((s.occ, s.tile), f32),
            pltpu.VMEM((s.tile, s.tile), bf),
            pltpu.VMEM((s.occ, s.pairs), f32),
            pltpu.VMEM((s.tile, s.tile), bf),
            pltpu.VMEM(flat_trial.shape, bf),
            pltpu.VMEM(flat_trial.shape, bf),
            pltpu.VMEM((s.thirds, s.local, s.parts * s.tiles, ROWS, s.slab), bf),
            pltpu.VMEM((s.thirds, s.parts - 1, s.local, s.tiles, ROWS, s.slab), bf),
            pltpu.VMEM((s.parts, s.thirds, s.local, s.tiles, ROWS, s.slab), bf),
            pltpu.VMEM((s.roots,) + wide_tile, bf),
            pltpu.VMEM((2, s.half, s.batch, ROWS, s.piece), bf),
            pltpu.VMEM((2, s.slots, s.batch, ROWS, s.piece), f32),
            pltpu.VMEM((s.slots,) + wide_tile, bf),
            pltpu.VMEM((s.slots,) + wide_tile, bf),
            pltpu.VMEM((s.slots,) + wide_tile, bf),
            pltpu.VMEM(flat_trial.shape, f32),
            pltpu.VMEM(trial.shape, bf),
            pltpu.VMEM((s.per * s.thirds, s.local) + third_tile, bf),
            pltpu.VMEM((s.thirds, s.local) + third_tile, bf),
            pltpu.VMEM((s.thirds, s.slots) + third_tile, bf),
            pltpu.VMEM((s.thirds, s.slots) + third_tile, bf),
            pltpu.VMEM((s.thirds, s.local) + third_tile, bf),
            pltpu.VMEM((s.thirds, s.local) + third_tile, bf),
            pltpu.VMEM((n, s.half * ROWS), f32),
            pltpu.VMEM((n, s.slots * ROWS), f32),
            pltpu.VMEM((CORES, ROWS, 128), f32),
            pltpu.VMEM((s.parts, ROWS, 128), f32),
            pltpu.VMEM((s.groups, ROWS, 128), f32),
            dma((s.groups,)), dma((s.groups,)),
            dma((s.per, s.local)), dma((s.roots,)), dma((s.groups,)), dma(()),
            dma(()), dma(()),
            dma((s.thirds, s.parts, s.local)), dma((s.thirds, s.parts, s.local)),
            dma((s.thirds, s.parts)), dma((s.thirds, s.parts)),
            dma((2,)), dma((s.steps,)), dma((s.steps,)),
            dma((s.thirds,)), dma((s.thirds,)),
            dma((s.thirds,)), dma((s.thirds,)),
            dma((s.thirds,)), dma((s.thirds,)),
            dma((s.thirds,)), dma((s.thirds,)),
            dma((s.thirds, s.local, s.per)),
            dma((CORES + s.parts + s.groups,)), dma((CORES + s.parts + s.groups,)),
        ],
        compiler_params=pltpu.CompilerParams(
            collective_id=0, has_side_effects=True, vmem_limit_bytes=66 * 1000 * 1000
        ),
        cost_estimate=pl.CostEstimate(
            flops=8 * s.rows * s.pairs * s.pairs, bytes_accessed=4 * w_ovoo.size, transcendentals=0
        ),
        name="sigma_step",
    )(converged, trial_singles, trial, flat_trial, occ_fock, fock, outer_in, coupling_in)
    return (sigma.reshape(trial_doubles.shape), singles, matrix)


def solution(mesh):
    placed = (
        P("root", None),
        P("root", "virt", "occ"),
        P(),
        P(),
        P("occ", "virt", "root"),
        P("occ", "virt", "root"),
        P(),
    )
    return jax.shard_map(
        local,
        mesh=mesh,
        in_specs=placed,
        out_specs=(P("root", "virt", "occ"), P("root", None), P("root", None)),
        check_vma=False,
    )
```
